32 devices in a mesh: dp: 16 (over z, y, core), tensor: 2 (over x).
Axes of the slice: x: 2, y: 2, z: 4, core: 2. Of those that a mesh axis runs over, the one named last changes fastest.
Arguments:
- tokens: bfloat16 [64, 144, 1024], P('dp', 'tensor'), may hold values from -150 to 150
- cotangent: bfloat16 [64, 144, 1024], P('dp', 'tensor'), may hold values from -6 to 6
- dispatch_weight: bfloat16 [1024, 32], replicated, may hold values from -3 to 3
- w_in: bfloat16 [32, 1024, 4096], P('dp', None, 'tensor'), may hold values from -0.1875 to 0.1875
- w_out: bfloat16 [32, 4096, 1024], P('dp', 'tensor'), may hold values from -0.09375 to 0.09375
Outputs:
- grad_tokens: bfloat16 [64, 144, 1024], P('dp', 'tensor')
- grad_router: float32 [1024, 32], replicated
- grad_w_in: bfloat16 [32, 1024, 4096], P('dp', None, 'tensor')
- grad_w_out: bfloat16 [32, 4096, 1024], P('dp', 'tensor')
The draws below stay inside these ranges and needn't reach their ends.
All inputs are finite; a program needn't handle non-finite values.
Results may differ from the reference program's by a relative error of at most 0.0079.
Values may be sent and summed in bfloat16 or wider, within the bound.
A program may use at most 64 MiB of HBM per device.

```python
import math
import jax
import jax.numpy as jnp
from jax import lax

D = 1024
FF = 4096
EXPERTS = 32
IMAGES = 64
SEQ = 144


def drawn_pair(key):
    router_key = jax.random.fold_in(key, 101)
    token_key = jax.random.fold_in(key, 102)
    router = jnp.clip(jax.random.normal(router_key, (D, EXPERTS), jnp.float32), -6.0, 6.0) * (3.0 / math.sqrt(D))
    base = jnp.clip(jax.random.normal(token_key, (IMAGES, SEQ, D), jnp.float32), -6.0, 6.0)
    position = jnp.arange(SEQ, dtype=jnp.float32) / max(SEQ - 1, 1)
    base = base * (0.6 * 3.0 ** position)[None, :, None]
    return (base, router)


def draw_tokens(key, part):
    return drawn_pair(key)[0].astype(jnp.bfloat16)


def draw_dispatch_weight(key, part):
    return drawn_pair(key)[1].astype(jnp.bfloat16)


def block_levels(own_key, dims, cuts, smallest, largest):
    gain = 1.0
    for axis_at, shards_of in cuts:
        draws = jax.random.uniform(jax.random.fold_in(jax.random.fold_in(own_key, 6), axis_at), (shards_of,), jnp.float32, smallest / len(cuts), largest / len(cuts))
        gain = gain * jnp.repeat(jnp.exp(draws), dims[axis_at] // shards_of).reshape((-1,) + (1,) * (len(dims) - 1 - axis_at))
    return gain


def bell_draw(own_key, dims, width, reach, split=(), kind=jnp.bfloat16):
    entries = jax.random.normal(own_key, dims, jnp.float32) * width
    if len(split) > 0:
        entries = block_levels(own_key, dims, split, -0.22, 0.18) * entries
    return jnp.clip(entries, min=-reach, max=reach).astype(kind)


def setup_inputs(seed: int = 0) -> dict:
    seeds = jax.random.split(jax.random.key(seed), 6)
    tokens = draw_tokens(jax.random.fold_in(seeds[5], 71), 0)
    cotangent = bell_draw(seeds[1], (IMAGES, SEQ, D), 1.0, 6.0, ((0, 16), (1, 2)))
    dispatch_weight = draw_dispatch_weight(jax.random.fold_in(seeds[5], 71), 0)
    w_in = bell_draw(seeds[3], (EXPERTS, D, FF), D ** -0.5, 0.1875, ((0, 16), (2, 2)))
    w_out = bell_draw(seeds[4], (EXPERTS, FF, D), FF ** -0.5, 0.09375, ((0, 16), (1, 2)))
    return dict(tokens=tokens, cotangent=cotangent, dispatch_weight=dispatch_weight, w_in=w_in, w_out=w_out)


def rounded(values):
    return lax.optimization_barrier(values.astype(jnp.bfloat16)).astype(jnp.float32)

def expert_forward(operands):
    slot_rows, first_mat, second_mat = operands
    pre_act = jnp.einsum('id,df->if', slot_rows, first_mat.astype(jnp.float32))
    hidden_low = rounded(jax.nn.gelu(pre_act))
    return jnp.einsum('if,fd->id', hidden_low, second_mat.astype(jnp.float32)).astype(jnp.bfloat16)

def expert_backward(operands):
    slot_rows, grad_rows, first_mat, second_mat = operands
    first_wide = first_mat.astype(jnp.float32)
    second_wide = second_mat.astype(jnp.float32)
    pre_act = jnp.einsum('id,df->if', slot_rows, first_wide)
    hidden_act, gelu_back = jax.vjp(jax.nn.gelu, pre_act)
    hidden_low = rounded(hidden_act)
    grad_hidden = jnp.einsum('id,fd->if', grad_rows, second_wide)
    grad_pre = rounded(gelu_back(grad_hidden)[0])
    grad_second = jnp.einsum('if,id->fd', hidden_low, grad_rows).astype(jnp.bfloat16)
    grad_first = jnp.einsum('id,if->df', slot_rows, grad_pre).astype(jnp.bfloat16)
    grad_slot = jnp.einsum('if,df->id', grad_pre, first_wide).astype(jnp.bfloat16)
    return (grad_first, grad_second, grad_slot)

def reference(tokens, cotangent, dispatch_weight, w_in, w_out):
    token_vals = tokens.astype(jnp.float32)
    grad_vals = cotangent.astype(jnp.float32)
    router = dispatch_weight.astype(jnp.float32)
    logits = jnp.einsum('isd,de->ise', token_vals, router)
    dispatch = jax.nn.softmax(logits, axis=1)
    combine = jax.nn.softmax(logits, axis=2)
    dispatch_low = rounded(dispatch)
    combine_low = rounded(combine)
    slot_inputs = rounded(jnp.einsum('ise,isd->ied', dispatch_low, token_vals))
    slot_major = jnp.transpose(slot_inputs, (1, 0, 2))
    slot_outputs = lax.map(expert_forward, (slot_major, w_in, w_out))
    slot_outputs = jnp.transpose(slot_outputs, (1, 0, 2)).astype(jnp.float32)
    grad_combine = jnp.einsum('isd,ied->ise', grad_vals, slot_outputs)
    grad_slots_out = rounded(jnp.einsum('ise,isd->ied', combine_low, grad_vals))
    grad_major = jnp.transpose(grad_slots_out, (1, 0, 2))
    grad_w_in, grad_w_out, grad_slots_in = lax.map(expert_backward, (slot_major, grad_major, w_in, w_out))
    grad_slots_in = jnp.transpose(grad_slots_in, (1, 0, 2)).astype(jnp.float32)
    grad_dispatch = jnp.einsum('isd,ied->ise', token_vals, grad_slots_in)
    row_dot = lax.optimization_barrier(jnp.sum(grad_combine * combine, axis=2, keepdims=True))
    column_dot = lax.optimization_barrier(jnp.sum(grad_dispatch * dispatch, axis=1, keepdims=True))
    grad_logits = rounded(combine * (grad_combine - row_dot) + dispatch * (grad_dispatch - column_dot))
    grad_tokens = (jnp.einsum('ise,ied->isd', dispatch_low, grad_slots_in) + jnp.einsum('ise,de->isd', grad_logits, router)).astype(jnp.bfloat16)
    grad_router = jnp.einsum('isd,ise->de', token_vals, grad_logits)
    return (grad_tokens, grad_router, grad_w_in, grad_w_out)
```

```python
import functools

import jax
import jax.numpy as jnp
from jax import lax
from jax.experimental import pallas as pl
from jax.experimental.pallas import tpu as pltpu
from jax.sharding import PartitionSpec as P

MESH = pl.DeviceIdType.MESH


def exchange_kernel(
    groups, shards, x_ref, out_ref, arrived, summed,
    near_send, near_recv, far_send, far_recv, pass_send, pass_recv,
):
    me = lax.axis_index("dp")
    part = lax.axis_index("tensor")

    def group_at(offset):
        return lax.rem(me + offset, groups)

    def shard_at(offset):
        return lax.rem(part + offset, shards)

    barrier = pltpu.get_barrier_semaphore()
    for k in range(1, shards):
        pl.semaphore_signal(barrier, inc=1, device_id=(me, shard_at(k)), device_id_type=MESH)

    def greet(o, carry):
        pl.semaphore_signal(barrier, inc=1, device_id=(group_at(o), part), device_id_type=MESH)
        return carry

    lax.fori_loop(1, groups, greet, 0)
    pl.semaphore_wait(barrier, shards - 1 + groups - 1)

    def near(k, o):
        return pltpu.make_async_remote_copy(
            src_ref=x_ref.at[shard_at(k), group_at(o)],
            dst_ref=arrived.at[k - 1, o],
            send_sem=near_send.at[k - 1, o],
            recv_sem=near_recv.at[k - 1, o],
            device_id=(me, shard_at(k)),
            device_id_type=MESH,
        )

    def far(o):
        return pltpu.make_async_remote_copy(
            src_ref=summed.at[o],
            dst_ref=out_ref.at[part, me],
            send_sem=far_send.at[o],
            recv_sem=far_recv.at[o],
            device_id=(group_at(o), part),
            device_id_type=MESH,
        )

    def passed(k, o):
        source = group_at(groups - o)
        return pltpu.make_async_remote_copy(
            src_ref=out_ref.at[part, source],
            dst_ref=out_ref.at[part, source],
            send_sem=pass_send.at[k - 1, o],
            recv_sem=pass_recv.at[k - 1, o],
            device_id=(me, shard_at(k)),
            device_id_type=MESH,
        )

    def add_up(o):
        total = x_ref[part, group_at(o)].astype(jnp.float32)
        for k in range(1, shards):
            near(k, o).wait_recv()
            total = total + arrived[k - 1, o].astype(jnp.float32)
        return total.astype(out_ref.dtype)

    def send_near(o, carry):
        for k in range(1, shards):
            near(k, lax.rem(o, groups)).start()
        return carry

    lax.fori_loop(1, groups + 1, send_near, 0)

    def send_far(o, carry):
        summed[o] = add_up(o)
        far(o).start()
        return carry

    lax.fori_loop(1, groups, send_far, 0)
    out_ref[part, me] = add_up(0)
    for k in range(1, shards):
        passed(k, 0).start()

    def pass_on(o, carry):
        far(o).wait_recv()
        for k in range(1, shards):
            passed(k, o).start()
        return carry

    lax.fori_loop(1, groups, pass_on, 0)

    def finish(o, carry):
        for k in range(1, shards):
            near(k, o).wait_send()
            passed(k, o).wait_send()
            passed(k, o).wait_recv()
        return carry

    lax.fori_loop(0, groups, finish, 0)

    def finish_far(o, carry):
        far(o).wait_send()
        return carry

    lax.fori_loop(1, groups, finish_far, 0)


def exchange(x, collective_id):
    shards, groups, rows, columns = x.shape
    vmem = pl.BlockSpec(memory_space=pltpu.VMEM)
    near_shape = (max(shards - 1, 1), groups)
    return pl.pallas_call(
        functools.partial(exchange_kernel, groups, shards),
        out_shape=jax.ShapeDtypeStruct(x.shape, x.dtype),
        in_specs=[vmem],
        out_specs=vmem,
        scratch_shapes=[
            pltpu.VMEM(near_shape + (rows, columns), x.dtype),
            pltpu.VMEM((groups, rows, columns), x.dtype),
            pltpu.SemaphoreType.DMA(near_shape),
            pltpu.SemaphoreType.DMA(near_shape),
            pltpu.SemaphoreType.DMA((groups,)),
            pltpu.SemaphoreType.DMA((groups,)),
            pltpu.SemaphoreType.DMA(near_shape),
            pltpu.SemaphoreType.DMA(near_shape),
        ],
        compiler_params=pltpu.CompilerParams(collective_id=collective_id, has_side_effects=True),
        name=f"exchange_{collective_id}",
    )(x)


def total_kernel(groups, shards, x_ref, out_ref, arrived, send, recv, back_send, back_recv):
    devices = groups * shards
    me = lax.axis_index("dp") * shards + lax.axis_index("tensor")

    def target(o):
        to = lax.rem(me + o, devices)
        return to, (to // shards, lax.rem(to, shards))

    barrier = pltpu.get_barrier_semaphore()

    def greet(o, carry):
        pl.semaphore_signal(barrier, inc=1, device_id=target(o)[1], device_id_type=MESH)
        return carry

    lax.fori_loop(1, devices, greet, 0)
    pl.semaphore_wait(barrier, devices - 1)

    def out_copy(o):
        to, place = target(o)
        return pltpu.make_async_remote_copy(
            src_ref=x_ref.at[to],
            dst_ref=arrived.at[o],
            send_sem=send.at[o],
            recv_sem=recv.at[o],
            device_id=place,
            device_id_type=MESH,
        )

    def back_copy(o):
        return pltpu.make_async_remote_copy(
            src_ref=out_ref.at[me],
            dst_ref=out_ref.at[me],
            send_sem=back_send.at[o],
            recv_sem=back_recv.at[o],
            device_id=target(o)[1],
            device_id_type=MESH,
        )

    def begin(o, carry):
        out_copy(o).start()
        return carry

    lax.fori_loop(1, devices, begin, 0)

    def add(o, total):
        out_copy(o).wait_recv()
        return total + arrived[o]

    out_ref[me] = lax.fori_loop(1, devices, add, x_ref[me])

    def give(o, carry):
        back_copy(o).start()
        return carry

    lax.fori_loop(1, devices, give, 0)

    def finish(o, carry):
        out_copy(o).wait_send()
        back_copy(o).wait_send()
        back_copy(o).wait_recv()
        return carry

    lax.fori_loop(1, devices, finish, 0)


def total_over_mesh(x, groups, shards, collective_id):
    devices = groups * shards
    blocks = x.reshape(devices, -1, 128)
    vmem = pl.BlockSpec(memory_space=pltpu.VMEM)
    out = pl.pallas_call(
        functools.partial(total_kernel, groups, shards),
        out_shape=jax.ShapeDtypeStruct(blocks.shape, blocks.dtype),
        in_specs=[vmem],
        out_specs=vmem,
        scratch_shapes=[
            pltpu.VMEM(blocks.shape, blocks.dtype),
            pltpu.SemaphoreType.DMA((devices,)),
            pltpu.SemaphoreType.DMA((devices,)),
            pltpu.SemaphoreType.DMA((devices,)),
            pltpu.SemaphoreType.DMA((devices,)),
        ],
        compiler_params=pltpu.CompilerParams(collective_id=collective_id, has_side_effects=True),
        name="router_total",
    )(blocks)
    return out.reshape(x.shape)


def to_experts(rows, groups, shards, collective_id):
    count = len(rows)
    images, experts, width = rows[0].shape
    own, columns = experts // groups, width // shards
    x = jnp.stack([r.astype(jnp.bfloat16) for r in rows])
    x = x.reshape(count, images, groups, own, shards, columns)
    x = x.transpose(4, 2, 0, 3, 1, 5).reshape(shards, groups, -1, columns)
    y = exchange(x, collective_id).reshape(shards, groups, count, own, images, columns)
    y = y.transpose(2, 3, 1, 4, 0, 5).reshape(count, own, groups * images, width)
    return [y[k] for k in range(count)]


def to_images(rows, groups, shards, collective_id):
    count = len(rows)
    own, everyone, width = rows[0].shape
    images, columns = everyone // groups, width // shards
    x = jnp.stack([r.astype(jnp.bfloat16) for r in rows])
    x = x.reshape(count, own, groups, images, shards, columns)
    x = x.transpose(4, 2, 0, 3, 1, 5).reshape(shards, groups, -1, columns)
    y = exchange(x, collective_id).reshape(shards, groups, count, images, own, columns)
    y = y.transpose(2, 3, 1, 4, 0, 5).reshape(count, images, groups * own, width)
    return [y[k] for k in range(count)]


def dispatch_softmax(logits):
    local_max = jnp.max(logits, axis=1)
    local_sum = jnp.sum(jnp.exp(logits - local_max[:, None, :]), axis=1)
    both = lax.all_gather(jnp.stack([local_max, local_sum]), "tensor")
    global_max = jnp.max(both[:, 0], axis=0)
    totals = jnp.sum(both[:, 1] * jnp.exp(both[:, 0] - global_max), axis=0)
    return jnp.exp(logits - global_max[:, None, :]) / totals[:, None, :]


def on_device(groups, shards, tokens, cotangent, dispatch_weight, w_in, w_out):
    wide = jnp.float32
    logits = jnp.einsum("isd,de->ise", tokens, dispatch_weight, preferred_element_type=wide)
    dispatch = dispatch_softmax(logits)
    combine = jax.nn.softmax(logits, axis=2)
    dispatch_low = dispatch.astype(jnp.bfloat16)
    combine_low = combine.astype(jnp.bfloat16)
    slot_inputs, grad_slots_out = to_experts(
        [
            jnp.einsum("ise,isd->ied", dispatch_low, tokens, preferred_element_type=wide),
            jnp.einsum("ise,isd->ied", combine_low, cotangent, preferred_element_type=wide),
        ],
        groups, shards, 0,
    )
    pre_act = jnp.einsum("eid,edf->eif", slot_inputs, w_in, preferred_element_type=wide)
    hidden_act, gelu_back = jax.vjp(jax.nn.gelu, pre_act)
    hidden_low = hidden_act.astype(jnp.bfloat16)
    grad_hidden = jnp.einsum("eid,efd->eif", grad_slots_out, w_out, preferred_element_type=wide)
    grad_pre = gelu_back(grad_hidden)[0].astype(jnp.bfloat16)
    slot_outputs, grad_slots_in = to_images(
        [
            jnp.einsum("eif,efd->eid", hidden_low, w_out, preferred_element_type=wide),
            jnp.einsum("eif,edf->eid", grad_pre, w_in, preferred_element_type=wide),
        ],
        groups, shards, 1,
    )
    grad_w_out = jnp.einsum(
        "eif,eid->efd", hidden_low, grad_slots_out, preferred_element_type=wide
    ).astype(jnp.bfloat16)
    grad_w_in = jnp.einsum(
        "eid,eif->edf", slot_inputs, grad_pre, preferred_element_type=wide
    ).astype(jnp.bfloat16)
    grad_combine = jnp.einsum("isd,ied->ise", cotangent, slot_outputs, preferred_element_type=wide)
    grad_dispatch = jnp.einsum("isd,ied->ise", tokens, grad_slots_in, preferred_element_type=wide)
    column_dot = lax.psum(jnp.sum(grad_dispatch * dispatch, axis=1), "tensor")
    row_dot = jnp.sum(grad_combine * combine, axis=2, keepdims=True)
    grad_logits = (
        combine * (grad_combine - row_dot) + dispatch * (grad_dispatch - column_dot[:, None, :])
    ).astype(jnp.bfloat16)
    token_part = jnp.einsum(
        "ise,ied->isd", dispatch_low, grad_slots_in, preferred_element_type=wide
    )
    router_part = jnp.einsum(
        "ise,de->isd", grad_logits, dispatch_weight, preferred_element_type=wide
    )
    grad_tokens = (token_part + router_part).astype(jnp.bfloat16)
    local_router = jnp.einsum("isd,ise->ed", tokens, grad_logits, preferred_element_type=wide)
    grad_router = total_over_mesh(local_router, groups, shards, 2).T
    return (grad_tokens, grad_router, grad_w_in, grad_w_out)


def solution(mesh):
    return jax.shard_map(
        functools.partial(on_device, mesh.shape["dp"], mesh.shape["tensor"]),
        mesh=mesh,
        in_specs=(
            P("dp", "tensor", None),
            P("dp", "tensor", None),
            P(),
            P("dp", None, "tensor"),
            P("dp", "tensor", None),
        ),
        out_specs=(P("dp", "tensor", None), P(), P("dp", None, "tensor"), P("dp", "tensor", None)),
        check_vma=False,
    )
```

```python
import functools

import jax
import jax.numpy as jnp
from jax import lax
from jax.experimental import pallas as pl
from jax.experimental.pallas import tpu as pltpu
from jax.sharding import PartitionSpec as P

MESH = pl.DeviceIdType.MESH
WAIT_COST = pl.CostEstimate(flops=18_000_000_000, bytes_accessed=50_000_000, transcendentals=0)


def exchange_kernel(
    groups, shards, x_ref, out_ref, arrived, summed,
    near_send, near_recv, far_send, far_recv, pass_send, pass_recv,
):
    me = lax.axis_index("dp")
    part = lax.axis_index("tensor")

    def group_at(offset):
        return lax.rem(me + offset, groups)

    def shard_at(offset):
        return lax.rem(part + offset, shards)

    barrier = pltpu.get_barrier_semaphore()
    for k in range(1, shards):
        pl.semaphore_signal(barrier, inc=1, device_id=(me, shard_at(k)), device_id_type=MESH)

    def greet(o, carry):
        pl.semaphore_signal(barrier, inc=1, device_id=(group_at(o), part), device_id_type=MESH)
        return carry

    lax.fori_loop(1, groups, greet, 0)
    pl.semaphore_wait(barrier, shards - 1 + groups - 1)

    def near(k, o):
        return pltpu.make_async_remote_copy(
            src_ref=x_ref.at[shard_at(k), group_at(o)],
            dst_ref=arrived.at[k - 1, o],
            send_sem=near_send.at[k - 1, o],
            recv_sem=near_recv.at[k - 1, o],
            device_id=(me, shard_at(k)),
            device_id_type=MESH,
        )

    def far(o):
        return pltpu.make_async_remote_copy(
            src_ref=summed.at[o],
            dst_ref=out_ref.at[part, me],
            send_sem=far_send.at[o],
            recv_sem=far_recv.at[o],
            device_id=(group_at(o), part),
            device_id_type=MESH,
        )

    def passed(k, o):
        source = group_at(groups - o)
        return pltpu.make_async_remote_copy(
            src_ref=out_ref.at[part, source],
            dst_ref=out_ref.at[part, source],
            send_sem=pass_send.at[k - 1, o],
            recv_sem=pass_recv.at[k - 1, o],
            device_id=(me, shard_at(k)),
            device_id_type=MESH,
        )

    def add_up(o):
        total = x_ref[part, group_at(o)].astype(jnp.float32)
        for k in range(1, shards):
            near(k, o).wait_recv()
            total = total + arrived[k - 1, o].astype(jnp.float32)
        return total.astype(out_ref.dtype)

    def send_near(o, carry):
        for k in range(1, shards):
            near(k, lax.rem(o, groups)).start()
        return carry

    lax.fori_loop(1, groups + 1, send_near, 0)

    def send_far(o, carry):
        summed[o] = add_up(o)
        far(o).start()
        return carry

    lax.fori_loop(1, groups, send_far, 0)
    out_ref[part, me] = add_up(0)
    for k in range(1, shards):
        passed(k, 0).start()

    def pass_on(o, carry):
        far(o).wait_recv()
        for k in range(1, shards):
            passed(k, o).start()
        return carry

    lax.fori_loop(1, groups, pass_on, 0)

    def finish(o, carry):
        for k in range(1, shards):
            near(k, o).wait_send()
            passed(k, o).wait_send()
            passed(k, o).wait_recv()
        return carry

    lax.fori_loop(0, groups, finish, 0)

    def finish_far(o, carry):
        far(o).wait_send()
        return carry

    lax.fori_loop(1, groups, finish_far, 0)


def grant(x, copies):
    return copies * x.size * x.dtype.itemsize + 2**20


def exchange(x, collective_id):
    shards, groups, rows, columns = x.shape
    vmem = pl.BlockSpec(memory_space=pltpu.VMEM)
    near_shape = (max(shards - 1, 1), groups)
    return pl.pallas_call(
        functools.partial(exchange_kernel, groups, shards),
        out_shape=jax.ShapeDtypeStruct(x.shape, x.dtype),
        in_specs=[vmem],
        out_specs=vmem,
        scratch_shapes=[
            pltpu.VMEM(near_shape + (rows, columns), x.dtype),
            pltpu.VMEM((groups, rows, columns), x.dtype),
            pltpu.SemaphoreType.DMA(near_shape),
            pltpu.SemaphoreType.DMA(near_shape),
            pltpu.SemaphoreType.DMA((groups,)),
            pltpu.SemaphoreType.DMA((groups,)),
            pltpu.SemaphoreType.DMA(near_shape),
            pltpu.SemaphoreType.DMA(near_shape),
        ],
        compiler_params=pltpu.CompilerParams(
            collective_id=collective_id, has_side_effects=True, vmem_limit_bytes=grant(x, 6)
        ),
        cost_estimate=WAIT_COST,
        name=f"exchange_{collective_id}",
    )(x)


def total_kernel(groups, shards, x_ref, out_ref, arrived, send, recv, back_send, back_recv):
    devices = groups * shards
    me = lax.axis_index("dp") * shards + lax.axis_index("tensor")

    def target(o):
        to = lax.rem(me + o, devices)
        return to, (to // shards, lax.rem(to, shards))

    barrier = pltpu.get_barrier_semaphore()

    def greet(o, carry):
        pl.semaphore_signal(barrier, inc=1, device_id=target(o)[1], device_id_type=MESH)
        return carry

    lax.fori_loop(1, devices, greet, 0)
    pl.semaphore_wait(barrier, devices - 1)

    def out_copy(o):
        to, place = target(o)
        return pltpu.make_async_remote_copy(
            src_ref=x_ref.at[to],
            dst_ref=arrived.at[o],
            send_sem=send.at[o],
            recv_sem=recv.at[o],
            device_id=place,
            device_id_type=MESH,
        )

    def back_copy(o):
        return pltpu.make_async_remote_copy(
            src_ref=out_ref.at[me],
            dst_ref=out_ref.at[me],
            send_sem=back_send.at[o],
            recv_sem=back_recv.at[o],
            device_id=target(o)[1],
            device_id_type=MESH,
        )

    def begin(o, carry):
        out_copy(o).start()
        return carry

    lax.fori_loop(1, devices, begin, 0)

    def add(o, total):
        out_copy(o).wait_recv()
        return total + arrived[o]

    out_ref[me] = lax.fori_loop(1, devices, add, x_ref[me])

    def give(o, carry):
        back_copy(o).start()
        return carry

    lax.fori_loop(1, devices, give, 0)

    def finish(o, carry):
        out_copy(o).wait_send()
        back_copy(o).wait_send()
        back_copy(o).wait_recv()
        return carry

    lax.fori_loop(1, devices, finish, 0)


def total_over_mesh(x, groups, shards, collective_id):
    devices = groups * shards
    experts, width = x.shape
    rows = experts * width // (devices * 128)
    blocks = x.reshape(experts // rows, rows, width // 128, 128).transpose(0, 2, 1, 3)
    blocks = blocks.reshape(devices, rows, 128)
    vmem = pl.BlockSpec(memory_space=pltpu.VMEM)
    out = pl.pallas_call(
        functools.partial(total_kernel, groups, shards),
        out_shape=jax.ShapeDtypeStruct(blocks.shape, blocks.dtype),
        in_specs=[vmem],
        out_specs=vmem,
        scratch_shapes=[
            pltpu.VMEM(blocks.shape, blocks.dtype),
            pltpu.SemaphoreType.DMA((devices,)),
            pltpu.SemaphoreType.DMA((devices,)),
            pltpu.SemaphoreType.DMA((devices,)),
            pltpu.SemaphoreType.DMA((devices,)),
        ],
        compiler_params=pltpu.CompilerParams(
            collective_id=collective_id, has_side_effects=True, vmem_limit_bytes=grant(blocks, 6)
        ),
        cost_estimate=WAIT_COST,
        name="router_total",
    )(blocks)
    out = out.reshape(experts // rows, width // 128, rows, 128).transpose(0, 2, 1, 3)
    return out.reshape(x.shape)


def outer_kernel(a_ref, b_ref, out_ref):
    out_ref[0] = lax.dot_general(
        a_ref[0], b_ref[0], (((0,), (0,)), ((), ())), preferred_element_type=jnp.float32
    ).astype(out_ref.dtype)


def outer_sums(a, b, tile):
    experts, images, m = a.shape
    n = b.shape[2]
    return pl.pallas_call(
        outer_kernel,
        grid=(experts, m // tile),
        in_specs=[
            pl.BlockSpec((1, images, tile), lambda e, k: (e, 0, k)),
            pl.BlockSpec((1, images, n), lambda e, k: (e, 0, 0)),
        ],
        out_specs=pl.BlockSpec((1, tile, n), lambda e, k: (e, k, 0)),
        out_shape=jax.ShapeDtypeStruct((experts, m, n), a.dtype),
        compiler_params=pltpu.CompilerParams(vmem_limit_bytes=12 * 2**20),
        cost_estimate=pl.CostEstimate(
            flops=2 * experts * images * m * n, bytes_accessed=2 * experts * m * n, transcendentals=0
        ),
        name="outer_sums",
    )(a, b)


def to_experts(rows, groups, shards, collective_id):
    count = len(rows)
    images, experts, width = rows[0].shape
    own, columns = experts // groups, width // shards
    x = jnp.stack([r.astype(jnp.bfloat16) for r in rows])
    x = x.reshape(count, images, groups, own, shards, columns)
    x = x.transpose(4, 2, 0, 3, 1, 5).reshape(shards, groups, -1, columns)
    y = exchange(x, collective_id).reshape(shards, groups, count, own, images, columns)
    y = y.transpose(2, 3, 1, 4, 0, 5).reshape(count, own, groups * images, width)
    return [y[k] for k in range(count)]


def to_images(rows, groups, shards, collective_id):
    count = len(rows)
    own, everyone, width = rows[0].shape
    images, columns = everyone // groups, width // shards
    x = jnp.stack([r.astype(jnp.bfloat16) for r in rows])
    x = x.reshape(count, own, groups, images, shards, columns)
    x = x.transpose(4, 2, 0, 3, 1, 5).reshape(shards, groups, -1, columns)
    y = exchange(x, collective_id).reshape(shards, groups, count, images, own, columns)
    y = y.transpose(2, 3, 1, 4, 0, 5).reshape(count, images, groups * own, width)
    return [y[k] for k in range(count)]


def dispatch_softmax(logits):
    local_max = jnp.max(logits, axis=1)
    local_sum = jnp.sum(jnp.exp(logits - local_max[:, None, :]), axis=1)
    both = lax.all_gather(jnp.stack([local_max, local_sum]), "tensor")
    global_max = jnp.max(both[:, 0], axis=0)
    totals = jnp.sum(both[:, 1] * jnp.exp(both[:, 0] - global_max), axis=0)
    return jnp.exp(logits - global_max[:, None, :]) / totals[:, None, :]


def on_device(groups, shards, tokens, cotangent, dispatch_weight, w_in, w_out):
    wide = jnp.float32
    logits = jnp.einsum("isd,de->ise", tokens, dispatch_weight, preferred_element_type=wide)
    dispatch = dispatch_softmax(logits)
    combine = jax.nn.softmax(logits, axis=2)
    dispatch_low = dispatch.astype(jnp.bfloat16)
    combine_low = combine.astype(jnp.bfloat16)
    slot_inputs, grad_slots_out = to_experts(
        [
            jnp.einsum("ise,isd->ied", dispatch_low, tokens, preferred_element_type=wide),
            jnp.einsum("ise,isd->ied", combine_low, cotangent, preferred_element_type=wide),
        ],
        groups, shards, 0,
    )
    pre_act = jnp.einsum("eid,edf->eif", slot_inputs, w_in, preferred_element_type=wide)
    hidden_act, gelu_back = jax.vjp(jax.nn.gelu, pre_act)
    hidden_low = hidden_act.astype(jnp.bfloat16)
    grad_hidden = jnp.einsum("eid,efd->eif", grad_slots_out, w_out, preferred_element_type=wide)
    grad_pre = gelu_back(grad_hidden)[0].astype(jnp.bfloat16)
    slot_outputs, grad_slots_in = to_images(
        [
            jnp.einsum("eif,efd->eid", hidden_low, w_out, preferred_element_type=wide),
            jnp.einsum("eif,edf->eid", grad_pre, w_in, preferred_element_type=wide),
        ],
        groups, shards, 1,
    )
    grad_w_out = outer_sums(hidden_low, grad_slots_out, min(512, hidden_low.shape[2]))
    grad_w_in = outer_sums(slot_inputs, grad_pre, min(256, slot_inputs.shape[2]))
    grad_combine = jnp.einsum("isd,ied->ise", cotangent, slot_outputs, preferred_element_type=wide)
    grad_dispatch = jnp.einsum("isd,ied->ise", tokens, grad_slots_in, preferred_element_type=wide)
    column_dot = lax.psum(jnp.sum(grad_dispatch * dispatch, axis=1), "tensor")
    row_dot = jnp.sum(grad_combine * combine, axis=2, keepdims=True)
    grad_logits = (
        combine * (grad_combine - row_dot) + dispatch * (grad_dispatch - column_dot[:, None, :])
    ).astype(jnp.bfloat16)
    token_part = jnp.einsum(
        "ise,ied->isd", dispatch_low, grad_slots_in, preferred_element_type=wide
    )
    router_part = jnp.einsum(
        "ise,de->isd", grad_logits, dispatch_weight, preferred_element_type=wide
    )
    grad_tokens = (token_part + router_part).astype(jnp.bfloat16)
    local_router = jnp.einsum("isd,ise->ed", tokens, grad_logits, preferred_element_type=wide)
    grad_router = total_over_mesh(local_router, groups, shards, 2).T
    return (grad_tokens, grad_router, grad_w_in, grad_w_out)


def solution(mesh):
    return jax.shard_map(
        functools.partial(on_device, mesh.shape["dp"], mesh.shape["tensor"]),
        mesh=mesh,
        in_specs=(
            P("dp", "tensor", None),
            P("dp", "tensor", None),
            P(),
            P("dp", None, "tensor"),
            P("dp", "tensor", None),
        ),
        out_specs=(P("dp", "tensor", None), P(), P("dp", None, "tensor"), P("dp", "tensor", None)),
        check_vma=False,
    )
```
